32 devices in a mesh: seq: 8 (over y, x, core), head: 4 (over z).
Axes of the slice: x: 2, y: 2, z: 4, core: 2. Of those that a mesh axis runs over, the one named last changes fastest.
Arguments:
- tokens: bfloat16 [32, 1024, 1024], P('seq'), may hold values from -6 to 6
- w_query: bfloat16 [1024, 1024], P(None, 'head'), may hold values from -1 to 1
- w_key: bfloat16 [1024, 1024], P(None, 'head'), may hold values from -1 to 1
- w_value: bfloat16 [1024, 1024], P(None, 'head'), may hold values from -0.1875 to 0.1875
- w_out: bfloat16 [1024, 1024], P('head'), may hold values from -0.1875 to 0.1875
Outputs:
- mixed: bfloat16 [32, 1024, 1024], P('seq', None, 'head')
The draws below stay inside these ranges and needn't reach their ends.
All inputs are finite; a program needn't handle non-finite values.
Results may differ from the reference program's by a relative error of at most 0.012.
Values may be sent and summed in bfloat16 or wider, within the bound.
A program may use at most 128 MiB of HBM per device.

```python
import jax
import jax.numpy as jnp
from jax import lax

D = 1024
HEADS = 16
FRAMES = 32
PATCHES = 1024


def query_key_pair(key):
    shape_full = (D, D)
    base = jnp.clip(jax.random.normal(jax.random.fold_in(key, 11), shape_full, jnp.float32), -6.0, 6.0)
    other = jnp.clip(jax.random.normal(jax.random.fold_in(key, 12), shape_full, jnp.float32), -6.0, 6.0)
    return (base * D ** (-0.5), other * D ** (-0.5))


def draw_w_query(key, part):
    first, second = query_key_pair(key)
    return first.astype(jnp.bfloat16)


def draw_w_key(key, part):
    first, second = query_key_pair(key)
    return second.astype(jnp.bfloat16)


def steps_of(own_key, extent, shards, low, high):
    level = 1.0
    for dim, parts in shards:
        draws = jax.random.uniform(jax.random.fold_in(jax.random.fold_in(own_key, 6), dim), (parts,), jnp.float32, low / len(shards), high / len(shards))
        level = level * jnp.repeat(jnp.exp(draws), extent[dim] // parts).reshape((-1,) + (1,) * (len(extent) - 1 - dim))
    return level


def noise(rng, extent, spread, limit, split=(), dtype=jnp.bfloat16):
    array = spread * jax.random.normal(rng, extent, jnp.float32)
    if split:
        array = array * steps_of(rng, extent, split, -0.22, 0.18)
    return jnp.clip(array, -limit, limit).astype(dtype)


def setup_inputs(seed: int = 0) -> dict:
    streams_of = jax.random.split(jax.random.key(seed), 6)
    tokens = noise(streams_of[0], (FRAMES, PATCHES, D), 1.0, 6.0, ((0, 8),))
    w_query = draw_w_query(jax.random.fold_in(streams_of[5], 71), 0)
    w_key = draw_w_key(jax.random.fold_in(streams_of[5], 71), 0)
    w_value = noise(streams_of[3], (D, D), D ** -0.5, 0.1875, ((1, 4),))
    w_out = noise(streams_of[4], (D, D), D ** -0.5, 0.1875, ((0, 4),))
    return {"tokens": tokens, "w_query": w_query, "w_key": w_key, "w_value": w_value, "w_out": w_out}


epsilon = 1e-05

def normalize(tokens):
    values = tokens.astype(jnp.float32)
    row_mean = lax.optimization_barrier(jnp.mean(values, axis=-1, keepdims=True))
    centered = values - row_mean
    row_var = lax.optimization_barrier(jnp.mean(centered * centered, axis=-1, keepdims=True))
    return (centered * lax.rsqrt(row_var + epsilon)).astype(jnp.bfloat16)

def project(source, weight):
    frames, patch_count, width = source.shape
    flat = jnp.dot(source.reshape(frames * patch_count, width), weight, preferred_element_type=jnp.float32)
    return flat.astype(jnp.bfloat16).reshape(frames, patch_count, weight.shape[1])

def attend(queries, key_rows, value_rows, head_count):
    frames, patch_count, feature_width = queries.shape
    head_size = feature_width // head_count
    query_flat = queries.reshape(frames, patch_count * head_count, head_size).astype(jnp.float32)
    key_flat = key_rows.reshape(frames, patch_count * head_count, head_size).astype(jnp.float32)
    value_flat = value_rows.reshape(frames, patch_count * head_count, head_size).astype(jnp.float32)
    scores = jnp.einsum('fmd,gmd->fgm', query_flat, key_flat) * head_size ** (-0.5)
    row_top = lax.optimization_barrier(jnp.max(scores, axis=1, keepdims=True))
    raised = jnp.exp(scores - row_top)
    weights = (raised / lax.optimization_barrier(jnp.sum(raised, axis=1, keepdims=True))).astype(jnp.bfloat16)
    attended = jnp.einsum('fgm,gmd->fmd', weights.astype(jnp.float32), value_flat)
    return attended.astype(jnp.bfloat16).reshape(frames, patch_count, feature_width)

def reference(tokens, w_query, w_key, w_value, w_out):
    normed = normalize(tokens)
    queries = project(normed, w_query)
    key_rows = project(normed, w_key)
    value_rows = project(normed, w_value)
    attended = attend(queries, key_rows, value_rows, HEADS)
    return project(attended, w_out)
```

```python
import functools

import jax
import jax.numpy as jnp
from jax import lax
from jax.experimental import pallas as pl
from jax.experimental.pallas import tpu as pltpu
from jax.sharding import PartitionSpec as P

HS = 64
EPSILON = 1e-05
SUB = 8
MASKED = -1e30
MESH = pl.DeviceIdType.MESH


def drain(ref, sem):
    pltpu.make_async_copy(ref, ref, sem).wait()


def grid_of(chips):
    tall = max(n for n in range(1, chips + 1) if chips % n == 0 and n * n <= chips)
    return tall, chips // tall


def kernel(
    seq, head,
    tok, wq, wk, wv, wo, out,
    x, normed, qkv, w, w_o, att, mixed, bias,
    tok_send, tok_recv, load_sem, z_send, z_recv, xy_send, xy_recv, far_recv, pair_recv,
    core_send, core_recv, out_send, out_recv,
):
    s, z = lax.axis_index("seq"), lax.axis_index("head")
    groups, frames = x.shape[0], x.shape[1]
    own_frames = tok.shape[0]
    width = tok.shape[2]
    columns = wq.shape[1]
    rows = frames * SUB
    own_patches = groups * SUB
    quarter = seq * own_patches
    slice_rows = width // seq
    half_rows = slice_rows // 2
    half_seq = seq // 2
    shard = width // head
    parity, place = lax.rem(s, 2), s // 2
    sibling = s + 1 - 2 * parity
    total = seq * head
    tall, wide = grid_of(half_seq)
    paired = tall == 2 and wide == 2
    up, across = place // wide, lax.rem(place, wide)
    colour = lax.rem(up + across, 2) if paired else 0
    colours = 2 if paired else 1
    sliced = (0, 1) if paired else (0, 1, 2)

    def send(src, dst, send_sem, recv_sem, to_s, to_z):
        pltpu.make_async_remote_copy(
            src_ref=src, dst_ref=dst, send_sem=send_sem, recv_sem=recv_sem,
            device_id=(to_s, to_z), device_id_type=MESH,
        ).start()

    def device_at(a, b):
        return (lax.rem(a, tall) * wide + lax.rem(b, wide)) * 2 + parity

    def slice_at(a, b, start, size):
        first = parity * half_seq + lax.rem(a, tall) * wide + lax.rem(b, wide)
        return pl.ds(pl.multiple_of(first * slice_rows + start, half_rows), size)

    def part(j):
        return (width if j < 3 else shard) // (2 * colours)

    def part_at(j, from_z, hue, start, size):
        first = (hue * 2 + parity) * part(j) + start
        if j < 3:
            return w.at[j, from_z, pl.ds(pl.multiple_of(first, size), size), :]
        return w_o.at[pl.ds(pl.multiple_of(from_z * shard + first, size), size), :]

    weights = (wq, wk, wv, wo)
    my_slice = slice_at(up, across, 0, slice_rows)

    def line_piece(j, from_z):
        if j in sliced:
            return w.at[j, from_z, my_slice, :]
        return part_at(j, from_z, colour, 0, part(j))

    def own_piece(j):
        if j in sliced:
            return weights[j].at[my_slice, :]
        start = pl.multiple_of((colour * 2 + parity) * part(j), part(j))
        return weights[j].at[pl.ds(start, part(j)), :]

    def ways(d):
        return (
            (z - d, z - d >= 0, z + 1, z + 1 < head),
            (z + d, z + d < head, z - 1, z - 1 >= 0),
        )

    def known(from_z):
        return jnp.clip(from_z, 0, head - 1)

    def launch(j):
        for _, _, after, open_ in ways(1):

            @pl.when(open_)
            def _():
                send(own_piece(j), line_piece(j, z), z_send.at[j], z_recv.at[j, z], s, after)

    def arrive(j, d):
        for from_z, valid, _, _ in ways(d):

            @pl.when(valid)
            def _():
                drain(line_piece(j, known(from_z)), z_recv.at[j, known(from_z)])

    def pass_on(j, d):
        for from_z, valid, after, open_ in ways(d):

            @pl.when(valid & open_)
            def _():
                piece = line_piece(j, known(from_z))
                send(piece, piece, z_send.at[j], z_recv.at[j, known(from_z)], s, after)

    def spread(j, d):
        for from_z, valid, _, _ in ways(d):
            f = known(from_z)

            @pl.when(valid)
            def _():
                piece = line_piece(j, f)
                if j in sliced:
                    for k in range(1, wide):
                        to_s = device_at(up, across + k)
                        send(piece, piece, xy_send.at[j], xy_recv.at[j, k - 1, f], to_s, z)
                    for k in range(1, tall):
                        to_s = device_at(up + k, across)
                        send(piece, piece, xy_send.at[j], xy_recv.at[j, wide + k - 2, f], to_s, z)
                    return
                if paired:
                    size = part(j) // 2
                    for i, to_s in ((0, device_at(up, across + 1)), (1, device_at(up + 1, across))):
                        some = part_at(j, f, colour, i * size, size)
                        send(some, some, xy_send.at[j], pair_recv.at[j - 2, i, f], to_s, z)
                send(piece, piece, core_send.at[j], core_recv.at[j], sibling, z)

    def relay(j, d):
        for from_z, valid, _, _ in ways(d):
            f = known(from_z)

            @pl.when(valid)
            def _():
                if j in sliced:
                    for k in range(1, wide):
                        b = across + wide - k
                        drain(w.at[j, f, slice_at(up, b, 0, slice_rows), :], xy_recv.at[j, k - 1, f])
                        some = w.at[j, f, slice_at(up, b, 0, half_rows), :]
                        for n in range(1, tall):
                            to_s = device_at(up + n, across)
                            send(some, some, xy_send.at[j], far_recv.at[j], to_s, z)
                    for k in range(1, tall):
                        a = up + tall - k
                        drain(
                            w.at[j, f, slice_at(a, across, 0, slice_rows), :],
                            xy_recv.at[j, wide + k - 2, f],
                        )
                        some = w.at[j, f, slice_at(a, across, half_rows, half_rows), :]
                        for n in range(1, wide):
                            to_s = device_at(up, across + n)
                            send(some, some, xy_send.at[j], far_recv.at[j], to_s, z)
                    return
                if paired:
                    size = part(j) // 2
                    for i in range(2):
                        some = part_at(j, f, 1 - colour, i * size, size)
                        drain(some, pair_recv.at[j - 2, i, f])
                        send(some, some, core_send.at[j], core_recv.at[j], sibling, z)

    far = (tall - 1) * (wide - 1) * slice_rows
    parity_rows = pl.ds(
        pl.multiple_of(parity * half_seq * slice_rows, slice_rows), half_seq * slice_rows
    )

    def to_sibling(j):
        if j not in sliced:
            return
        if far:
            drain(w.at[j, pl.ds(0, head - 1), pl.ds(0, far), :], far_recv.at[j])
        for i in range(1, head):
            piece = w.at[j, lax.rem(z + i, head), parity_rows, :]
            send(piece, piece, core_send.at[j], core_recv.at[j], sibling, z)

    def tok_block(to_s, g):
        start = pl.multiple_of(z * quarter + to_s * own_patches + g * SUB, SUB)
        return tok.at[:, pl.ds(start, SUB), :]

    def exchange(g):
        for i in range(1, seq):
            to_s = lax.rem(s + i, seq)
            send(
                tok_block(to_s, g), x.at[g, pl.ds(s * own_frames, own_frames)],
                tok_send.at[g], tok_recv.at[g], to_s, z,
            )

    def keep(g):
        pltpu.make_async_copy(
            tok_block(s, g), x.at[g, pl.ds(s * own_frames, own_frames)], tok_recv.at[g]
        ).start()

    barrier = pltpu.get_barrier_semaphore()
    for i in range(1, seq):
        pl.semaphore_signal(
            barrier, inc=1, device_id=(lax.rem(s + i, seq), z), device_id_type=MESH
        )
    for _, _, after, open_ in ways(1):

        @pl.when(open_)
        def _():
            pl.semaphore_signal(barrier, inc=1, device_id=(s, after), device_id_type=MESH)

    own = [pltpu.make_async_copy(weights[j], w.at[j, z], load_sem.at[j]) for j in range(3)]
    own.append(
        pltpu.make_async_copy(
            wo, w_o.at[pl.ds(pl.multiple_of(z * shard, shard), shard), :], load_sem.at[3]
        )
    )
    for copy in own:
        copy.start()
    keep(0)

    row = lax.broadcasted_iota(jnp.int32, (rows, rows), 0)
    col = lax.broadcasted_iota(jnp.int32, (rows, rows), 1)
    bias[...] = jnp.where((row & (SUB - 1)) == (col & (SUB - 1)), 0.0, MASKED)

    lines = (z > 0).astype(jnp.int32) + (z + 1 < head).astype(jnp.int32)
    pl.semaphore_wait(barrier, seq - 1 + lines)

    step_frames = 8

    def norm(g):
        drain(x.at[g], tok_recv.at[g])

        @pl.loop(0, frames // step_frames)
        def _(c):
            block = x[g, pl.ds(c * step_frames, step_frames)].astype(jnp.float32)
            values = block.reshape(step_frames * SUB, width)
            mean = jnp.mean(values, axis=-1, keepdims=True)
            centered = values - mean
            var = jnp.mean(centered * centered, axis=-1, keepdims=True)
            start = pl.multiple_of(c * step_frames * SUB, step_frames * SUB)
            normed[pl.ds(start, step_frames * SUB), :] = (
                centered * lax.rsqrt(var + EPSILON)
            ).astype(jnp.bfloat16)

    def project(j):
        @pl.loop(0, head, unroll=True)
        def _(h):
            r = jnp.dot(normed[...], w[j, h], preferred_element_type=jnp.float32)
            if j == 0:
                r = r * HS ** (-0.5)
            start = pl.multiple_of(h * columns, columns)
            qkv[j, :, pl.ds(start, columns)] = r.astype(jnp.bfloat16)

    def take(j):
        own[j].wait()
        if j < 3:
            drain(
                w.at[j, pl.ds(0, head - 1), pl.ds(0, width // 2), :], core_recv.at[j]
            )
            project(j)
        else:
            drain(w_o.at[pl.ds(0, (head - 1) * shard // 2), :], core_recv.at[j])

    pair = 2 * HS
    left = lax.broadcasted_iota(jnp.int32, (rows, pair), 1) < HS
    left_b = left.astype(jnp.float32).astype(jnp.bfloat16)
    right_b = (1.0 - left.astype(jnp.float32)).astype(jnp.bfloat16)
    ones = jnp.ones((rows, pair), jnp.bfloat16)

    def out_block(g):
        start = pl.multiple_of(z * quarter + s * own_patches + g * SUB, SUB)
        return out.at[:, pl.ds(start, SUB), :]

    def attend():
        @pl.loop(0, width // pair, unroll=4)
        def _(n):
            lanes = pl.ds(pl.multiple_of(n * pair, pair), pair)
            q, k, v = qkv[0, :, lanes], qkv[1, :, lanes], qkv[2, :, lanes]
            v_ones = jnp.concatenate([v, ones], axis=1)
            results = []
            for mask in (left_b, right_b):
                score = lax.dot_general(
                    q * mask, k, (((1,), (1,)), ((), ())), preferred_element_type=jnp.float32
                )
                score = score + bias[...]
                top = jnp.max(score, axis=1, keepdims=True)
                raised = jnp.exp(score - top).astype(jnp.bfloat16)
                r = jnp.dot(raised, v_ones, preferred_element_type=jnp.float32)
                results.append(r[:, :pair] / r[:, pair:])
            att[:, lanes] = jnp.where(left, results[0], results[1]).astype(jnp.bfloat16)

    if head == 4:
        order = (lax.rem(z + 2, 4), 3 - z, z + 1 - 2 * lax.rem(z, 2), z)
    else:
        order = tuple(lax.rem(z + k, head) for k in range(1, head + 1))

    def mix(g):
        for n, h in enumerate(order):
            lanes = pl.ds(pl.multiple_of(h * columns, columns), columns)
            r = jnp.dot(att[...], w_o[:, lanes], preferred_element_type=jnp.float32)
            mixed[g, pl.ds(h * frames, frames)] = r.reshape(frames, SUB, columns).astype(
                jnp.bfloat16
            )
            last = n == head - 1

            @pl.loop(1 if last else 0, seq)
            def _(i):
                to_s = lax.rem(s + i, seq)
                send(
                    mixed.at[g, pl.ds(h * frames + to_s * own_frames, own_frames)],
                    out_block(g), out_send.at[g], out_recv, to_s, h,
                )

        pltpu.make_async_copy(
            mixed.at[g, pl.ds(z * frames + s * own_frames, own_frames)], out_block(g), out_recv
        ).start()

    for j in range(3):
        launch(j)
    exchange(0)
    for j in (0, 1):
        arrive(j, 1)
        pass_on(j, 1)
        spread(j, 1)
    launch(3)
    arrive(2, 1)
    spread(2, 1)
    norm(0)
    for d in range(2, head):
        for j in (0, 1):
            arrive(j, d)
            pass_on(j, d)
            spread(j, d)
            relay(j, d - 1)
        if d == 2:
            pass_on(2, 1)
            arrive(3, 1)
            spread(3, 1)
    if head == 2:
        pass_on(2, 1)
        arrive(3, 1)
        spread(3, 1)
    for d in range(2, head):
        arrive(2, d)
        pass_on(2, d)
        spread(2, d)
        relay(2, d - 1)
        if d == 2:
            relay(0, head - 1)
            relay(1, head - 1)
            pass_on(3, 1)
            relay(3, 1)
    if head == 2:
        relay(0, 1)
        relay(1, 1)
        pass_on(3, 1)
    to_sibling(0)
    for d in range(2, head):
        arrive(3, d)
        pass_on(3, d)
        spread(3, d)
        if d == 2:
            to_sibling(1)
            relay(2, head - 1)
            to_sibling(2)
            take(0)
        if d > 2:
            relay(3, d - 1)
    if head == 2:
        to_sibling(1)
        relay(2, 1)
        to_sibling(2)
        take(0)
    for g in range(1, groups):
        exchange(g)
        keep(g)
    take(1)
    relay(3, head - 1)
    take(2)
    attend()
    take(3)
    mix(0)

    @pl.loop(1, groups)
    def _(g):
        norm(g)
        for j in range(3):
            project(j)
        attend()
        mix(g)

    drain(out, out_recv)
    blocks = head * frames
    for g in range(groups):
        drain(mixed.at[g, pl.ds(0, blocks - blocks // total)], out_send.at[g])
        drain(x.at[g, pl.ds(0, frames - own_frames)], tok_send.at[g])
    for j in range(4):
        for d in range(head):
            for from_z, valid, _, open_ in ways(d):

                @pl.when(valid & open_)
                def _():
                    drain(line_piece(j, known(from_z)), z_send.at[j])

        if j in sliced:
            spreads = (half_seq - 1) * slice_rows
        else:
            spreads = part(j) if paired else 0
        if j < 3:
            if spreads:
                drain(w.at[j, pl.ds(0, head - 1), pl.ds(0, spreads), :], xy_send.at[j])
            drain(w.at[j, pl.ds(0, head - 1), pl.ds(0, width // 2), :], core_send.at[j])
        else:
            if spreads:
                drain(w_o.at[pl.ds(0, (head - 1) * spreads), :], xy_send.at[j])
            drain(w_o.at[pl.ds(0, (head - 1) * shard // 2), :], core_send.at[j])


def local(tokens, w_query, w_key, w_value, w_out):
    seq, head = lax.axis_size("seq"), lax.axis_size("head")
    own_frames, patches, width = tokens.shape
    frames = own_frames * seq
    groups = patches // (seq * head * SUB)
    rows = frames * SUB
    columns = w_query.shape[1]
    tall, wide = grid_of(seq // 2)
    bf16 = jnp.bfloat16
    dma = pltpu.SemaphoreType.DMA
    return pl.pallas_call(
        functools.partial(kernel, seq, head),
        out_shape=pltpu.VMEM((own_frames, patches, width // head), bf16),
        in_specs=[pl.BlockSpec(memory_space=pl.ANY)] * 5,
        out_specs=pl.BlockSpec(memory_space=pl.ANY),
        scratch_shapes=[
            pltpu.VMEM((groups, frames, SUB, width), bf16),
            pltpu.VMEM((rows, width), bf16),
            pltpu.VMEM((3, rows, width), bf16),
            pltpu.VMEM((3, head, width, columns), bf16),
            pltpu.VMEM((width, width), bf16),
            pltpu.VMEM((rows, width), bf16),
            pltpu.VMEM((groups, head * frames, SUB, width // head), bf16),
            pltpu.VMEM((rows, rows), jnp.float32),
            dma((groups,)), dma((groups,)), dma((4,)),
            dma((4,)), dma((4, head)), dma((4,)), dma((3, max(tall + wide - 2, 1), head)), dma((3,)),
            dma((2, 2, head)), dma((4,)), dma((4,)), dma((groups,)), dma,
        ],
        compiler_params=pltpu.CompilerParams(
            has_side_effects=True, collective_id=0, vmem_limit_bytes=58 * 1024 * 1024
        ),
    )(tokens, w_query, w_key, w_value, w_out)


def solution(mesh):
    return jax.shard_map(
        local,
        mesh=mesh,
        in_specs=(
            P("seq", None, None),
            P(None, "head"),
            P(None, "head"),
            P(None, "head"),
            P("head", None),
        ),
        out_specs=P("seq", None, "head"),
        check_vma=False,
    )
```

```python
import functools

import jax
import jax.numpy as jnp
from jax import lax
from jax.experimental import pallas as pl
from jax.experimental.pallas import tpu as pltpu
from jax.sharding import PartitionSpec as P

HS = 64
EPSILON = 1e-05
SUB = 8
MASKED = -1e30
MESH = pl.DeviceIdType.MESH


def drain(ref, sem):
    pltpu.make_async_copy(ref, ref, sem).wait()


def grid_of(chips):
    tall = max(n for n in range(1, chips + 1) if chips % n == 0 and n * n <= chips)
    return tall, chips // tall


def kernel(
    seq, head,
    tok, wq, wk, wv, wo, out,
    x, normed, qkv, w, w_o, att, mixed, bias,
    tok_send, tok_recv, load_sem, z_send, z_recv, xy_send, xy_recv, far_recv, pair_recv,
    core_send, core_recv, out_send, out_recv,
):
    s, z = lax.axis_index("seq"), lax.axis_index("head")
    groups, frames = x.shape[0], x.shape[1]
    own_frames = tok.shape[0]
    width = tok.shape[2]
    columns = wq.shape[1]
    rows = frames * SUB
    own_patches = groups * SUB
    quarter = seq * own_patches
    slice_rows = width // seq
    half_rows = slice_rows // 2
    half_seq = seq // 2
    shard = width // head
    parity, place = lax.rem(s, 2), s // 2
    sibling = s + 1 - 2 * parity
    total = seq * head
    tall, wide = grid_of(half_seq)
    paired = tall == 2 and wide == 2
    up, across = place // wide, lax.rem(place, wide)
    colour = lax.rem(up + across, 2) if paired else 0
    colours = 2 if paired else 1
    sliced = (0, 1) if paired else (0, 1, 2)

    def send(src, dst, send_sem, recv_sem, to_s, to_z):
        pltpu.make_async_remote_copy(
            src_ref=src, dst_ref=dst, send_sem=send_sem, recv_sem=recv_sem,
            device_id=(to_s, to_z), device_id_type=MESH,
        ).start()

    def device_at(a, b):
        return (lax.rem(a, tall) * wide + lax.rem(b, wide)) * 2 + parity

    def slice_at(a, b, start, size):
        first = parity * half_seq + lax.rem(a, tall) * wide + lax.rem(b, wide)
        return pl.ds(pl.multiple_of(first * slice_rows + start, half_rows), size)

    def part(j):
        return (width if j < 3 else shard) // (2 * colours)

    def part_at(j, from_z, hue, start, size):
        first = (hue * 2 + parity) * part(j) + start
        if j < 3:
            return w.at[j, from_z, pl.ds(pl.multiple_of(first, size), size), :]
        return w_o.at[pl.ds(pl.multiple_of(from_z * shard + first, size), size), :]

    weights = (wq, wk, wv, wo)
    my_slice = slice_at(up, across, 0, slice_rows)

    def line_piece(j, from_z):
        if j in sliced:
            return w.at[j, from_z, my_slice, :]
        return part_at(j, from_z, colour, 0, part(j))

    def own_piece(j):
        if j in sliced:
            return weights[j].at[my_slice, :]
        start = pl.multiple_of((colour * 2 + parity) * part(j), part(j))
        return weights[j].at[pl.ds(start, part(j)), :]

    def ways(d):
        return (
            (z - d, z - d >= 0, z + 1, z + 1 < head),
            (z + d, z + d < head, z - 1, z - 1 >= 0),
        )

    def known(from_z):
        return jnp.clip(from_z, 0, head - 1)

    inner = (z > 0) & (z + 1 < head)

    def whole(j, from_z, to_z):
        if not paired:
            return z < 0
        deep = (to_z > 0) & (to_z + 1 < head)
        if j == 3:
            return z < 0
        if j == 2:
            return deep
        return deep & ((from_z == 0) | (from_z == head - 1))

    def launch(j):
        for _, _, after, open_ in ways(1):

            @pl.when(open_)
            def _():
                send(own_piece(j), line_piece(j, z), z_send.at[j], z_recv.at[j, z], s, after)

    def complete(j):
        if not paired:
            return
        for _, _, after, open_ in ways(1):

            @pl.when(open_ & whole(j, z, after))
            def _():
                if j in sliced:
                    places = (
                        ((0, 1), xy_recv.at[j, 0, z]), ((1, 0), xy_recv.at[j, 1, z]),
                        ((1, 1), far_recv.at[j]),
                    )
                    for (a, b), arrived in places:
                        some = slice_at(up + a, across + b, 0, slice_rows)
                        send(
                            weights[j].at[some, :], w.at[j, z, some, :],
                            z_send.at[j], arrived, s, after,
                        )
                else:
                    size = part(j) // 2
                    for i in range(2):
                        first = ((1 - colour) * 2 + parity) * part(j) + i * size
                        send(
                            weights[j].at[pl.ds(pl.multiple_of(first, size), size), :],
                            part_at(j, z, 1 - colour, i * size, size),
                            z_send.at[j], pair_recv.at[j - 2, i, z], s, after,
                        )

    def picked(from_z, outer):
        edge = (from_z == 0) | (from_z == head - 1)
        if outer is None:
            return True
        return edge if outer else jnp.logical_not(edge)

    def arrive(j, d, outer=None):
        for from_z, valid, _, _ in ways(d):

            @pl.when(valid & picked(from_z, outer))
            def _():
                drain(line_piece(j, known(from_z)), z_recv.at[j, known(from_z)])

    def pass_on(j, d, outer=None):
        for from_z, valid, after, open_ in ways(d):

            @pl.when(valid & open_ & picked(from_z, outer))
            def _():
                piece = line_piece(j, known(from_z))
                send(piece, piece, z_send.at[j], z_recv.at[j, known(from_z)], s, after)

    def spread(j, d, outer=None):
        for from_z, valid, _, _ in ways(d):
            f = known(from_z)
            valid = valid & picked(from_z, outer)
            thin = valid & jnp.logical_not(whole(j, from_z, z)) if d == 1 else valid
            piece = line_piece(j, f)

            @pl.when(thin)
            def _():
                if j in sliced:
                    for k in range(1, wide):
                        to_s = device_at(up, across + k)
                        send(piece, piece, xy_send.at[j], xy_recv.at[j, k - 1, f], to_s, z)
                    for k in range(1, tall):
                        to_s = device_at(up + k, across)
                        send(piece, piece, xy_send.at[j], xy_recv.at[j, wide + k - 2, f], to_s, z)
                elif paired:
                    size = part(j) // 2
                    for i, to_s in ((0, device_at(up, across + 1)), (1, device_at(up + 1, across))):
                        some = part_at(j, f, colour, i * size, size)
                        send(some, some, xy_send.at[j], pair_recv.at[j - 2, i, f], to_s, z)

            if j not in sliced:

                @pl.when(valid)
                def _():
                    send(piece, piece, core_send.at[j], core_recv.at[j], sibling, z)

    def relay(j, d, full=False):
        for from_z, valid, _, _ in ways(d):
            f = known(from_z)
            if d == 1:
                is_whole = whole(j, from_z, z)
                chosen = valid & (is_whole if full else jnp.logical_not(is_whole))
            elif full:
                continue
            else:
                chosen = valid

            @pl.when(chosen)
            def _():
                if j in sliced:
                    for k in range(1, wide):
                        b = across + wide - k
                        drain(w.at[j, f, slice_at(up, b, 0, slice_rows), :], xy_recv.at[j, k - 1, f])
                        some = w.at[j, f, slice_at(up, b, 0, half_rows), :]
                        for n in range(1, 1 if full else tall):
                            to_s = device_at(up + n, across)
                            send(some, some, xy_send.at[j], far_recv.at[j], to_s, z)
                    for k in range(1, tall):
                        a = up + tall - k
                        drain(
                            w.at[j, f, slice_at(a, across, 0, slice_rows), :],
                            xy_recv.at[j, wide + k - 2, f],
                        )
                        some = w.at[j, f, slice_at(a, across, half_rows, half_rows), :]
                        for n in range(1, 1 if full else wide):
                            to_s = device_at(up, across + n)
                            send(some, some, xy_send.at[j], far_recv.at[j], to_s, z)
                    return
                if paired:
                    size = part(j) // 2
                    for i in range(2):
                        some = part_at(j, f, 1 - colour, i * size, size)
                        drain(some, pair_recv.at[j - 2, i, f])
                        send(some, some, core_send.at[j], core_recv.at[j], sibling, z)

    far = (tall - 1) * (wide - 1) * slice_rows
    parity_rows = pl.ds(
        pl.multiple_of(parity * half_seq * slice_rows, slice_rows), half_seq * slice_rows
    )

    def to_sibling(j):
        if j not in sliced:
            return
        if far:
            drain(w.at[j, pl.ds(0, head - 1), pl.ds(0, far), :], far_recv.at[j])
        for i in range(1, head):
            piece = w.at[j, lax.rem(z + i, head), parity_rows, :]
            send(piece, piece, core_send.at[j], core_recv.at[j], sibling, z)

    def tok_block(to_s, g):
        start = pl.multiple_of(z * quarter + to_s * own_patches + g * SUB, SUB)
        return tok.at[:, pl.ds(start, SUB), :]

    def exchange(g):
        for i in range(1, seq):
            to_s = lax.rem(s + i, seq)
            send(
                tok_block(to_s, g), x.at[g, pl.ds(s * own_frames, own_frames)],
                tok_send.at[g], tok_recv.at[g], to_s, z,
            )

    def keep(g):
        pltpu.make_async_copy(
            tok_block(s, g), x.at[g, pl.ds(s * own_frames, own_frames)], tok_recv.at[g]
        ).start()

    barrier = pltpu.get_barrier_semaphore()
    for i in range(1, seq):
        pl.semaphore_signal(
            barrier, inc=1, device_id=(lax.rem(s + i, seq), z), device_id_type=MESH
        )
    for _, _, after, open_ in ways(1):

        @pl.when(open_)
        def _():
            pl.semaphore_signal(barrier, inc=1, device_id=(s, after), device_id_type=MESH)

    own = [pltpu.make_async_copy(weights[j], w.at[j, z], load_sem.at[j]) for j in range(3)]
    own.append(
        pltpu.make_async_copy(
            wo, w_o.at[pl.ds(pl.multiple_of(z * shard, shard), shard), :], load_sem.at[3]
        )
    )
    for copy in own:
        copy.start()
    keep(0)

    row = lax.broadcasted_iota(jnp.int32, (rows, rows), 0)
    col = lax.broadcasted_iota(jnp.int32, (rows, rows), 1)
    bias[...] = jnp.where((row & (SUB - 1)) == (col & (SUB - 1)), 0.0, MASKED)

    lines = (z > 0).astype(jnp.int32) + (z + 1 < head).astype(jnp.int32)
    pl.semaphore_wait(barrier, seq - 1 + lines)

    step_frames = 8

    def norm(g):
        drain(x.at[g], tok_recv.at[g])

        @pl.loop(0, frames // step_frames)
        def _(c):
            block = x[g, pl.ds(c * step_frames, step_frames)].astype(jnp.float32)
            values = block.reshape(step_frames * SUB, width)
            mean = jnp.mean(values, axis=-1, keepdims=True)
            centered = values - mean
            var = jnp.mean(centered * centered, axis=-1, keepdims=True)
            start = pl.multiple_of(c * step_frames * SUB, step_frames * SUB)
            normed[pl.ds(start, step_frames * SUB), :] = (
                centered * lax.rsqrt(var + EPSILON)
            ).astype(jnp.bfloat16)

    def project(j):
        @pl.loop(0, head, unroll=True)
        def _(h):
            r = jnp.dot(normed[...], w[j, h], preferred_element_type=jnp.float32)
            if j == 0:
                r = r * HS ** (-0.5)
            start = pl.multiple_of(h * columns, columns)
            qkv[j, :, pl.ds(start, columns)] = r.astype(jnp.bfloat16)

    def take(j):
        own[j].wait()
        if j < 3:
            drain(
                w.at[j, pl.ds(0, head - 1), pl.ds(0, width // 2), :], core_recv.at[j]
            )
            project(j)
        else:
            drain(w_o.at[pl.ds(0, (head - 1) * shard // 2), :], core_recv.at[j])

    pair = 2 * HS
    left = lax.broadcasted_iota(jnp.int32, (rows, pair), 1) < HS
    left_b = left.astype(jnp.float32).astype(jnp.bfloat16)
    right_b = (1.0 - left.astype(jnp.float32)).astype(jnp.bfloat16)
    ones = jnp.ones((rows, pair), jnp.bfloat16)

    def out_block(g):
        start = pl.multiple_of(z * quarter + s * own_patches + g * SUB, SUB)
        return out.at[:, pl.ds(start, SUB), :]

    pairs = width // pair
    some = pairs // 2

    def attend(start, stop):
        @pl.loop(start, stop, unroll=4)
        def _(n):
            lanes = pl.ds(pl.multiple_of(n * pair, pair), pair)
            q, k, v = qkv[0, :, lanes], qkv[1, :, lanes], qkv[2, :, lanes]
            v_ones = jnp.concatenate([v, ones], axis=1)
            results = []
            for mask in (left_b, right_b):
                score = lax.dot_general(
                    q * mask, k, (((1,), (1,)), ((), ())), preferred_element_type=jnp.float32
                )
                score = score + bias[...]
                top = jnp.max(score, axis=1, keepdims=True)
                raised = jnp.exp(score - top).astype(jnp.bfloat16)
                r = jnp.dot(raised, v_ones, preferred_element_type=jnp.float32)
                results.append(r[:, :pair] / r[:, pair:])
            att[:, lanes] = jnp.where(left, results[0], results[1]).astype(jnp.bfloat16)

    if head == 4:
        order = (lax.rem(z + 2, 4), 3 - z, z + 1 - 2 * lax.rem(z, 2), z)
    else:
        order = tuple(lax.rem(z + k, head) for k in range(1, head + 1))

    def mix(g):
        for h in range(head):
            lanes = pl.ds(h * columns, columns)
            r = jnp.dot(att[...], w_o[:, lanes], preferred_element_type=jnp.float32)
            mixed[g, pl.ds(h * frames, frames)] = r.reshape(frames, SUB, columns).astype(
                jnp.bfloat16
            )
        for n, h in enumerate(order):

            @pl.loop(1 if n == head - 1 else 0, seq)
            def _(i):
                to_s = lax.rem(s + i, seq)
                send(
                    mixed.at[g, pl.ds(h * frames + to_s * own_frames, own_frames)],
                    out_block(g), out_send.at[g], out_recv, to_s, h,
                )

        pltpu.make_async_copy(
            mixed.at[g, pl.ds(z * frames + s * own_frames, own_frames)], out_block(g), out_recv
        ).start()

    for j in range(3):
        launch(j)
    exchange(0)

    @pl.when(jnp.logical_not(inner))
    def _():
        launch(3)
        for j in range(3):
            complete(j)

    for j in (0, 1):
        arrive(j, 1)
        pass_on(j, 1)
        spread(j, 1)

    def fetch(g):
        if g < groups:
            exchange(g)
            keep(g)

    def forward(j, d, outer=None):
        arrive(j, d, outer)
        pass_on(j, d, outer)
        spread(j, d, outer)

    @pl.when(inner)
    def _():
        launch(3)
        forward(2, 1, True)
        arrive(2, 1, False)
        spread(2, 1, False)
        norm(0)
        for d in range(2, head):
            for j in (0, 1):
                forward(j, d)
        pass_on(2, 1, False)
        forward(3, 1, True)
        for j in range(3):
            complete(j)
        for j in (0, 1):
            relay(j, 1)
        for j in (0, 1):
            for d in range(2, head):
                relay(j, d)
        for d in range(2, head):
            forward(2, d)
        forward(3, 1, False)
        relay(0, 1, True)
        to_sibling(0)
        for d in range(2, head):
            forward(3, d)
        relay(1, 1, True)
        to_sibling(1)
        fetch(1)
        take(0)
        relay(2, 1)
        for d in range(2, head):
            relay(2, d)
        take(1)
        relay(2, 1, True)
        to_sibling(2)
        relay(3, 1)
        take(2)
        attend(0, some)
        for d in range(2, head):
            relay(3, d)
        relay(3, 1, True)
        fetch(2)
        attend(some, pairs)
        take(3)
        mix(0)
        fetch(3)

    @pl.when(jnp.logical_not(inner))
    def _():
        arrive(2, 1)
        spread(2, 1)
        norm(0)
        for d in range(2, head):
            for j in (0, 1):
                arrive(j, d)
                spread(j, d)
                relay(j, d - 1)
            if d == 2:
                arrive(3, 1)
                spread(3, 1)
        if head == 2:
            arrive(3, 1)
            spread(3, 1)
        relay(2, 1)
        for d in range(2, head):
            arrive(2, d)
            spread(2, d)
            if d == 2:
                for j in (0, 1):
                    relay(j, head - 1)
                relay(3, 1)
        if head == 2:
            relay(0, 1)
            relay(1, 1)
        to_sibling(0)
        to_sibling(1)
        for d in range(2, head):
            arrive(3, d)
            spread(3, d)
            relay(2, d)
            if d == 2:
                take(0)
        if head == 2:
            take(0)
        to_sibling(2)
        take(1)
        for d in range(2, head - 1):
            relay(3, d)
        fetch(1)
        take(2)
        attend(0, some)
        fetch(2)
        if head > 2:
            relay(3, head - 1)
        else:
            relay(3, 1)
        attend(some, pairs)
        fetch(3)
        take(3)
        mix(0)

    for g in range(4, groups):
        fetch(g)

    @pl.loop(1, groups)
    def _(g):
        norm(g)
        for j in range(3):
            project(j)
        attend(0, pairs)
        mix(g)

    drain(out, out_recv)
    blocks = head * frames
    for g in range(groups):
        drain(mixed.at[g, pl.ds(0, blocks - blocks // total)], out_send.at[g])
        drain(x.at[g, pl.ds(0, frames - own_frames)], tok_send.at[g])
    for j in range(4):
        matrix = w.at[j, 0] if j < 3 else w_o

        def returned(count, sem):
            if count:
                drain(matrix.at[pl.ds(0, count), :], sem)

        if j in sliced:
            line, others, over = slice_rows, (half_seq - 1) * slice_rows, (half_seq - 1) * slice_rows
        else:
            line, others, over = part(j), part(j), part(j) if paired else 0
        for d in range(head):
            for from_z, valid, after, open_ in ways(d):

                @pl.when(valid & open_)
                def _():
                    returned(line, z_send.at[j])

                if d == 0:

                    @pl.when(open_ & whole(j, z, after))
                    def _():
                        returned(others, z_send.at[j])
                else:
                    thin = valid & jnp.logical_not(whole(j, from_z, z)) if d == 1 else valid

                    @pl.when(thin)
                    def _():
                        returned(over, xy_send.at[j])

        for _ in range(1, head):
            returned((width if j < 3 else shard) // 2, core_send.at[j])


def local(tokens, w_query, w_key, w_value, w_out):
    seq, head = lax.axis_size("seq"), lax.axis_size("head")
    own_frames, patches, width = tokens.shape
    frames = own_frames * seq
    groups = patches // (seq * head * SUB)
    rows = frames * SUB
    columns = w_query.shape[1]
    tall, wide = grid_of(seq // 2)
    bf16 = jnp.bfloat16
    dma = pltpu.SemaphoreType.DMA
    return pl.pallas_call(
        functools.partial(kernel, seq, head),
        out_shape=pltpu.VMEM((own_frames, patches, width // head), bf16),
        in_specs=[pl.BlockSpec(memory_space=pl.ANY)] * 5,
        out_specs=pl.BlockSpec(memory_space=pl.ANY),
        scratch_shapes=[
            pltpu.VMEM((groups, frames, SUB, width), bf16),
            pltpu.VMEM((rows, width), bf16),
            pltpu.VMEM((3, rows, width), bf16),
            pltpu.VMEM((3, head, width, columns), bf16),
            pltpu.VMEM((width, width), bf16),
            pltpu.VMEM((rows, width), bf16),
            pltpu.VMEM((groups, head * frames, SUB, width // head), bf16),
            pltpu.VMEM((rows, rows), jnp.float32),
            dma((groups,)), dma((groups,)), dma((4,)),
            dma((4,)), dma((4, head)), dma((4,)), dma((3, max(tall + wide - 2, 1), head)), dma((3,)),
            dma((2, 2, head)), dma((4,)), dma((4,)), dma((groups,)), dma,
        ],
        compiler_params=pltpu.CompilerParams(
            has_side_effects=True, collective_id=0, vmem_limit_bytes=58 * 1024 * 1024
        ),
    )(tokens, w_query, w_key, w_value, w_out)


def solution(mesh):
    return jax.shard_map(
        local,
        mesh=mesh,
        in_specs=(
            P("seq", None, None),
            P(None, "head"),
            P(None, "head"),
            P(None, "head"),
            P("head", None),
        ),
        out_specs=P("seq", None, "head"),
        check_vma=False,
    )
```

```python
import functools

import jax
import jax.numpy as jnp
from jax import lax
from jax.experimental import pallas as pl
from jax.experimental.pallas import tpu as pltpu
from jax.sharding import PartitionSpec as P

HS = 64
EPSILON = 1e-05
SUB = 8
MASKED = -1e30
MESH = pl.DeviceIdType.MESH


def drain(ref, sem):
    pltpu.make_async_copy(ref, ref, sem).wait()


def grid_of(chips):
    tall = max(n for n in range(1, chips + 1) if chips % n == 0 and n * n <= chips)
    return tall, chips // tall


def kernel(
    seq, head,
    tok, wq, wk, wv, wo, out,
    x, normed, qkv, w, w_o, att, mixed, bias,
    tok_send, tok_recv, load_sem, z_send, z_recv, xy_send, xy_recv, far_recv, pair_recv,
    core_send, core_recv, out_send, out_recv,
):
    s, z = lax.axis_index("seq"), lax.axis_index("head")
    slots, frames = x.shape[0], x.shape[1]
    groups = tok.shape[1] // (seq * head * SUB)
    own_frames = tok.shape[0]
    width = tok.shape[2]
    columns = wq.shape[1]
    rows = frames * SUB
    slice_rows = width // seq
    half_rows = slice_rows // 2
    half_seq = seq // 2
    shard = width // head
    parity, place = lax.rem(s, 2), s // 2
    sibling = s + 1 - 2 * parity
    total = seq * head
    tall, wide = grid_of(half_seq)
    paired = tall == 2 and wide == 2
    up, across = place // wide, lax.rem(place, wide)
    colour = lax.rem(up + across, 2) if paired else 0
    colours = 2 if paired else 1
    sliced = (0, 1) if paired else (0, 1, 2)

    def send(src, dst, send_sem, recv_sem, to_s, to_z):
        pltpu.make_async_remote_copy(
            src_ref=src, dst_ref=dst, send_sem=send_sem, recv_sem=recv_sem,
            device_id=(to_s, to_z), device_id_type=MESH,
        ).start()

    def device_at(a, b):
        return (lax.rem(a, tall) * wide + lax.rem(b, wide)) * 2 + parity

    def slice_at(a, b, start, size):
        first = parity * half_seq + lax.rem(a, tall) * wide + lax.rem(b, wide)
        return pl.ds(pl.multiple_of(first * slice_rows + start, half_rows), size)

    def part(j):
        return (width if j < 3 else shard) // (2 * colours)

    def part_at(j, from_z, hue, start, size):
        first = (hue * 2 + parity) * part(j) + start
        if j < 3:
            return w.at[j, from_z, pl.ds(pl.multiple_of(first, size), size), :]
        return w_o.at[pl.ds(pl.multiple_of(from_z * shard + first, size), size), :]

    weights = (wq, wk, wv, wo)
    my_slice = slice_at(up, across, 0, slice_rows)

    def line_piece(j, from_z):
        if j in sliced:
            return w.at[j, from_z, my_slice, :]
        return part_at(j, from_z, colour, 0, part(j))

    def own_piece(j):
        if j in sliced:
            return weights[j].at[my_slice, :]
        start = pl.multiple_of((colour * 2 + parity) * part(j), part(j))
        return weights[j].at[pl.ds(start, part(j)), :]

    def ways(d):
        return (
            (z - d, z - d >= 0, z + 1, z + 1 < head),
            (z + d, z + d < head, z - 1, z - 1 >= 0),
        )

    def known(from_z):
        return jnp.clip(from_z, 0, head - 1)

    inner = (z > 0) & (z + 1 < head)
    deep = inner.astype(jnp.int32)
    uneven = head == 4 and paired and groups == 4
    edge_groups, full, twice = (3, 5, 0) if uneven else (groups, groups, 0)

    def whole(j, from_z, to_z):
        if not paired:
            return z < 0
        deep = (to_z > 0) & (to_z + 1 < head)
        if j == 3:
            return z < 0
        if j == 2:
            return deep
        return deep & ((from_z == 0) | (from_z == head - 1))

    def launch(j):
        for _, _, after, open_ in ways(1):

            @pl.when(open_)
            def _():
                send(own_piece(j), line_piece(j, z), z_send.at[j], z_recv.at[j, z], s, after)

    def complete(j):
        if not paired:
            return
        for _, _, after, open_ in ways(1):

            @pl.when(open_ & whole(j, z, after))
            def _():
                if j in sliced:
                    places = (
                        ((0, 1), xy_recv.at[j, 0, z]), ((1, 0), xy_recv.at[j, 1, z]),
                        ((1, 1), far_recv.at[j]),
                    )
                    for (a, b), arrived in places:
                        some = slice_at(up + a, across + b, 0, slice_rows)
                        send(
                            weights[j].at[some, :], w.at[j, z, some, :],
                            z_send.at[j], arrived, s, after,
                        )
                else:
                    size = part(j) // 2
                    for i in range(2):
                        first = ((1 - colour) * 2 + parity) * part(j) + i * size
                        send(
                            weights[j].at[pl.ds(pl.multiple_of(first, size), size), :],
                            part_at(j, z, 1 - colour, i * size, size),
                            z_send.at[j], pair_recv.at[j - 2, i, z], s, after,
                        )

    def picked(from_z, outer):
        edge = (from_z == 0) | (from_z == head - 1)
        if outer is None:
            return True
        return edge if outer else jnp.logical_not(edge)

    def arrive(j, d, outer=None):
        for from_z, valid, _, _ in ways(d):

            @pl.when(valid & picked(from_z, outer))
            def _():
                drain(line_piece(j, known(from_z)), z_recv.at[j, known(from_z)])

    def pass_on(j, d, outer=None):
        for from_z, valid, after, open_ in ways(d):

            @pl.when(valid & open_ & picked(from_z, outer))
            def _():
                piece = line_piece(j, known(from_z))
                send(piece, piece, z_send.at[j], z_recv.at[j, known(from_z)], s, after)

    def spread(j, d, outer=None):
        for from_z, valid, _, _ in ways(d):
            f = known(from_z)
            valid = valid & picked(from_z, outer)
            thin = valid & jnp.logical_not(whole(j, from_z, z)) if d == 1 else valid
            piece = line_piece(j, f)

            @pl.when(thin)
            def _():
                if j in sliced:
                    for k in range(1, wide):
                        to_s = device_at(up, across + k)
                        send(piece, piece, xy_send.at[j], xy_recv.at[j, k - 1, f], to_s, z)
                    for k in range(1, tall):
                        to_s = device_at(up + k, across)
                        send(piece, piece, xy_send.at[j], xy_recv.at[j, wide + k - 2, f], to_s, z)
                elif paired:
                    size = part(j) // 2
                    for i, to_s in ((0, device_at(up, across + 1)), (1, device_at(up + 1, across))):
                        some = part_at(j, f, colour, i * size, size)
                        send(some, some, xy_send.at[j], pair_recv.at[j - 2, i, f], to_s, z)

            if j not in sliced:

                @pl.when(valid)
                def _():
                    send(piece, piece, core_send.at[j], core_recv.at[j], sibling, z)

    def relay(j, d, full=False):
        for from_z, valid, _, _ in ways(d):
            f = known(from_z)
            if d == 1:
                is_whole = whole(j, from_z, z)
                chosen = valid & (is_whole if full else jnp.logical_not(is_whole))
            elif full:
                continue
            else:
                chosen = valid

            @pl.when(chosen)
            def _():
                if j in sliced:
                    for k in range(1, wide):
                        b = across + wide - k
                        drain(w.at[j, f, slice_at(up, b, 0, slice_rows), :], xy_recv.at[j, k - 1, f])
                        some = w.at[j, f, slice_at(up, b, 0, half_rows), :]
                        for n in range(1, 1 if full else tall):
                            to_s = device_at(up + n, across)
                            send(some, some, xy_send.at[j], far_recv.at[j], to_s, z)
                    for k in range(1, tall):
                        a = up + tall - k
                        drain(
                            w.at[j, f, slice_at(a, across, 0, slice_rows), :],
                            xy_recv.at[j, wide + k - 2, f],
                        )
                        some = w.at[j, f, slice_at(a, across, half_rows, half_rows), :]
                        for n in range(1, 1 if full else wide):
                            to_s = device_at(up, across + n)
                            send(some, some, xy_send.at[j], far_recv.at[j], to_s, z)
                    return
                if paired:
                    size = part(j) // 2
                    for i in range(2):
                        some = part_at(j, f, 1 - colour, i * size, size)
                        drain(some, pair_recv.at[j - 2, i, f])
                        send(some, some, core_send.at[j], core_recv.at[j], sibling, z)

    far = (tall - 1) * (wide - 1) * slice_rows
    parity_rows = pl.ds(
        pl.multiple_of(parity * half_seq * slice_rows, slice_rows), half_seq * slice_rows
    )

    def to_sibling(j):
        if j not in sliced:
            return
        if far:
            drain(w.at[j, pl.ds(0, head - 1), pl.ds(0, far), :], far_recv.at[j])
        for i in range(1, head):
            piece = w.at[j, lax.rem(z + i, head), parity_rows, :]
            send(piece, piece, core_send.at[j], core_recv.at[j], sibling, z)

    def patches_of(to_s, g):
        if not uneven:
            block = (z * seq + to_s) * groups + g
        else:
            at_edge = ((z // (head - 1)) * seq + to_s) * edge_groups + g
            single = 2 * seq * edge_groups + ((z - 1) * seq + to_s) * full + g
            double = 2 * seq * (edge_groups + full) + to_s * twice + (g - full)
            late = int(g >= full) if isinstance(g, int) else (g >= full).astype(jnp.int32)
            block = at_edge + deep * (single + late * (double - single) - at_edge)
        return pl.ds(pl.multiple_of(block * SUB, SUB), SUB)

    def tok_block(to_s, g):
        return tok.at[:, patches_of(to_s, g), :]

    def exchange(g):
        for i in range(1, seq):
            to_s = lax.rem(s + i, seq)
            send(
                tok_block(to_s, g), x.at[g, pl.ds(s * own_frames, own_frames)],
                tok_send.at[g], tok_recv.at[g], to_s, z,
            )

    def keep(g):
        pltpu.make_async_copy(
            tok_block(s, g), x.at[g, pl.ds(s * own_frames, own_frames)], tok_recv.at[g]
        ).start()

    barrier = pltpu.get_barrier_semaphore()
    for i in range(1, seq):
        pl.semaphore_signal(
            barrier, inc=1, device_id=(lax.rem(s + i, seq), z), device_id_type=MESH
        )
    for _, _, after, open_ in ways(1):

        @pl.when(open_)
        def _():
            pl.semaphore_signal(barrier, inc=1, device_id=(s, after), device_id_type=MESH)

    own = [pltpu.make_async_copy(weights[j], w.at[j, z], load_sem.at[j]) for j in range(3)]
    own.append(
        pltpu.make_async_copy(
            wo, w_o.at[pl.ds(pl.multiple_of(z * shard, shard), shard), :], load_sem.at[3]
        )
    )
    for copy in own:
        copy.start()
    keep(0)

    row = lax.broadcasted_iota(jnp.int32, (rows, rows), 0)
    col = lax.broadcasted_iota(jnp.int32, (rows, rows), 1)
    bias[...] = jnp.where((row & (SUB - 1)) == (col & (SUB - 1)), 0.0, MASKED)

    lines = (z > 0).astype(jnp.int32) + (z + 1 < head).astype(jnp.int32)
    pl.semaphore_wait(barrier, seq - 1 + lines)

    step_frames = 8

    def norm(g):
        drain(x.at[g], tok_recv.at[g])

        @pl.loop(0, frames // step_frames, unroll=True)
        def _(c):
            block = x[g, pl.ds(c * step_frames, step_frames)].astype(jnp.float32)
            values = block.reshape(step_frames * SUB, width)
            mean = jnp.mean(values, axis=-1, keepdims=True)
            centered = values - mean
            var = jnp.mean(centered * centered, axis=-1, keepdims=True)
            start = pl.multiple_of(c * step_frames * SUB, step_frames * SUB)
            normed[pl.ds(start, step_frames * SUB), :] = (
                centered * lax.rsqrt(var + EPSILON)
            ).astype(jnp.bfloat16)

    def project(j):
        @pl.loop(0, head, unroll=True)
        def _(h):
            r = jnp.dot(normed[...], w[j, h], preferred_element_type=jnp.float32)
            if j == 0:
                r = r * HS ** (-0.5)
            start = pl.multiple_of(h * columns, columns)
            qkv[j, :, pl.ds(start, columns)] = r.astype(jnp.bfloat16)

    def take(j):
        own[j].wait()
        if j < 3:
            drain(
                w.at[j, pl.ds(0, head - 1), pl.ds(0, width // 2), :], core_recv.at[j]
            )
            project(j)
        else:
            drain(w_o.at[pl.ds(0, (head - 1) * shard // 2), :], core_recv.at[j])

    pair = 2 * HS
    left = lax.broadcasted_iota(jnp.int32, (rows, pair), 1) < HS
    left_b = left.astype(jnp.float32).astype(jnp.bfloat16)
    right_b = (1.0 - left.astype(jnp.float32)).astype(jnp.bfloat16)
    ones = jnp.ones((rows, pair), jnp.bfloat16)

    def out_block(g):
        return out.at[:, patches_of(s, g), :]

    pairs = width // pair
    some = pairs // 2

    def attend(start, stop):
        @pl.loop(start, stop, unroll=4)
        def _(n):
            lanes = pl.ds(pl.multiple_of(n * pair, pair), pair)
            q, k, v = qkv[0, :, lanes], qkv[1, :, lanes], qkv[2, :, lanes]
            v_ones = jnp.concatenate([v, ones], axis=1)
            results = []
            for mask in (left_b, right_b):
                score = lax.dot_general(
                    q * mask, k, (((1,), (1,)), ((), ())), preferred_element_type=jnp.float32
                )
                score = score + bias[...]
                top = jnp.max(score, axis=1, keepdims=True)
                raised = jnp.exp(score - top).astype(jnp.bfloat16)
                r = jnp.dot(raised, v_ones, preferred_element_type=jnp.float32)
                results.append(r[:, :pair] / r[:, pair:])
            att[:, lanes] = jnp.where(left, results[0], results[1]).astype(jnp.bfloat16)

    if head == 4:
        order = (lax.rem(z + 2, 4), 3 - z, z + 1 - 2 * lax.rem(z, 2), z)
    else:
        order = tuple(lax.rem(z + k, head) for k in range(1, head + 1))

    def blend(g, h):
        lanes = pl.ds(pl.multiple_of(h * columns, columns), columns)
        r = jnp.dot(att[...], w_o[:, lanes], preferred_element_type=jnp.float32)
        mixed[g, pl.ds(h * frames, frames)] = r.reshape(frames, SUB, columns).astype(jnp.bfloat16)

    def deliver(g, some_heads):
        for h in some_heads:

            @pl.loop(1 if h is z else 0, seq)
            def _(i):
                to_s = lax.rem(s + i, seq)
                send(
                    mixed.at[g, pl.ds(h * frames + to_s * own_frames, own_frames)],
                    out_block(g), out_send.at[g], out_recv, to_s, h,
                )

        pltpu.make_async_copy(
            mixed.at[g, pl.ds(z * frames + s * own_frames, own_frames)], out_block(g), out_recv
        ).start()

    def mix(g):
        for h in range(head):
            blend(g, h)
        deliver(g, order)

    def mix_half(g):
        for h in order[2:]:
            blend(g, h)
        deliver(g, order[2:])

    for j in range(3):
        launch(j)
    exchange(0)

    @pl.when(jnp.logical_not(inner))
    def _():
        launch(3)
        for j in range(3):
            complete(j)

    for j in (0, 1):
        arrive(j, 1)
        pass_on(j, 1)
        spread(j, 1)

    def fetch(g, count=edge_groups):
        if g < count:
            exchange(g)
            keep(g)

    def forward(j, d, outer=None):
        arrive(j, d, outer)
        pass_on(j, d, outer)
        spread(j, d, outer)

    @pl.when(inner)
    def _():
        launch(3)
        forward(2, 1, True)
        arrive(2, 1, False)
        spread(2, 1, False)
        norm(0)
        for d in range(2, head):
            for j in (0, 1):
                forward(j, d)
        pass_on(2, 1, False)
        forward(3, 1, True)
        for j in range(3):
            complete(j)
        for j in (0, 1):
            relay(j, 1)
        for j in (0, 1):
            for d in range(2, head):
                relay(j, d)
        for d in range(2, head):
            forward(2, d)
        forward(3, 1, False)
        relay(0, 1, True)
        to_sibling(0)
        for d in range(2, head):
            forward(3, d)
        relay(1, 1, True)
        to_sibling(1)
        fetch(1, full + twice)
        take(0)
        relay(2, 1)
        for d in range(2, head):
            relay(2, d)
        take(1)
        relay(2, 1, True)
        to_sibling(2)
        relay(3, 1)
        take(2)
        attend(0, some)
        for d in range(2, head):
            relay(3, d)
        relay(3, 1, True)
        fetch(2, full + twice)
        attend(some, pairs)
        take(3)
        mix(0)
        for g in range(3, slots):
            fetch(g, full + twice)

    @pl.when(jnp.logical_not(inner))
    def _():
        arrive(2, 1)
        spread(2, 1)
        norm(0)
        for d in range(2, head):
            for j in (0, 1):
                arrive(j, d)
                spread(j, d)
                relay(j, d - 1)
            if d == 2:
                arrive(3, 1)
                spread(3, 1)
        if head == 2:
            arrive(3, 1)
            spread(3, 1)
        relay(2, 1)
        for d in range(2, head):
            arrive(2, d)
            spread(2, d)
            if d == 2:
                for j in (0, 1):
                    relay(j, head - 1)
                relay(3, 1)
        if head == 2:
            relay(0, 1)
            relay(1, 1)
        to_sibling(0)
        to_sibling(1)
        for d in range(2, head):
            arrive(3, d)
            spread(3, d)
            relay(2, d)
            if d == 2:
                take(0)
        if head == 2:
            take(0)
        to_sibling(2)
        take(1)
        for d in range(2, head - 1):
            relay(3, d)
        fetch(1)
        take(2)
        attend(0, some)
        fetch(2)
        if head > 2:
            relay(3, head - 1)
        else:
            relay(3, 1)
        attend(some, pairs)
        fetch(3)
        take(3)
        mix(0)

    def prepare(g):
        norm(g)
        for j in range(3):
            project(j)
        attend(0, pairs)

    @pl.loop(1, edge_groups + deep * (full - edge_groups))
    def _(g):
        prepare(g)
        mix(g)

    if twice:

        @pl.loop(full, full + twice * deep)
        def _(g):
            prepare(g)
            mix_half(g)

    drain(out, out_recv)
    blocks = head * frames
    def sent(g, count):
        drain(mixed.at[g, pl.ds(0, count)], out_send.at[g])
        drain(x.at[g, pl.ds(0, frames - own_frames)], tok_send.at[g])

    every = blocks - blocks // total
    for g in range(min(edge_groups, full)):
        sent(g, every)
    if uneven:

        @pl.when(jnp.logical_not(inner))
        def _():
            for g in range(full, edge_groups):
                sent(g, every)

        @pl.when(inner)
        def _():
            for g in range(edge_groups, full):
                sent(g, every)
            for g in range(full, full + twice):
                sent(g, 2 * frames - own_frames)

    for j in range(4):
        matrix = w.at[j, 0] if j < 3 else w_o

        def returned(count, sem):
            if count:
                drain(matrix.at[pl.ds(0, count), :], sem)

        if j in sliced:
            line, others, over = slice_rows, (half_seq - 1) * slice_rows, (half_seq - 1) * slice_rows
        else:
            line, others, over = part(j), part(j), part(j) if paired else 0
        for d in range(head):
            for from_z, valid, after, open_ in ways(d):

                @pl.when(valid & open_)
                def _():
                    returned(line, z_send.at[j])

                if d == 0:

                    @pl.when(open_ & whole(j, z, after))
                    def _():
                        returned(others, z_send.at[j])
                else:
                    thin = valid & jnp.logical_not(whole(j, from_z, z)) if d == 1 else valid

                    @pl.when(thin)
                    def _():
                        returned(over, xy_send.at[j])

        for _ in range(1, head):
            returned((width if j < 3 else shard) // 2, core_send.at[j])


def local(tokens, w_query, w_key, w_value, w_out):
    seq, head = lax.axis_size("seq"), lax.axis_size("head")
    own_frames, patches, width = tokens.shape
    frames = own_frames * seq
    groups = patches // (seq * head * SUB)
    tall, wide = grid_of(seq // 2)
    rows = frames * SUB
    uneven = head == 4 and (tall, wide) == (2, 2) and groups == 4
    slots = 5 if uneven else groups
    columns = w_query.shape[1]
    bf16 = jnp.bfloat16
    dma = pltpu.SemaphoreType.DMA
    return pl.pallas_call(
        functools.partial(kernel, seq, head),
        out_shape=pltpu.VMEM((own_frames, patches, width // head), bf16),
        in_specs=[pl.BlockSpec(memory_space=pl.ANY)] * 5,
        out_specs=pl.BlockSpec(memory_space=pl.ANY),
        scratch_shapes=[
            pltpu.VMEM((slots, frames, SUB, width), bf16),
            pltpu.VMEM((rows, width), bf16),
            pltpu.VMEM((3, rows, width), bf16),
            pltpu.VMEM((3, head, width, columns), bf16),
            pltpu.VMEM((width, width), bf16),
            pltpu.VMEM((rows, width), bf16),
            pltpu.VMEM((slots, head * frames, SUB, width // head), bf16),
            pltpu.VMEM((rows, rows), jnp.float32),
            dma((slots,)), dma((slots,)), dma((4,)),
            dma((4,)), dma((4, head)), dma((4,)), dma((3, max(tall + wide - 2, 1), head)), dma((3,)),
            dma((2, 2, head)), dma((4,)), dma((4,)), dma((slots,)), dma,
        ],
        compiler_params=pltpu.CompilerParams(
            has_side_effects=True, collective_id=0, vmem_limit_bytes=58 * 1024 * 1024
        ),
    )(tokens, w_query, w_key, w_value, w_out)


def solution(mesh):
    return jax.shard_map(
        local,
        mesh=mesh,
        in_specs=(
            P("seq", None, None),
            P(None, "head"),
            P(None, "head"),
            P(None, "head"),
            P("head", None),
        ),
        out_specs=P("seq", None, "head"),
        check_vma=False,
    )
```

```python
import functools

import jax
import jax.numpy as jnp
from jax import lax
from jax.experimental import pallas as pl
from jax.experimental.pallas import tpu as pltpu
from jax.sharding import PartitionSpec as P

HS = 64
EPSILON = 1e-05
SUB = 8
MASKED = -1e30
MESH = pl.DeviceIdType.MESH


def drain(ref, sem):
    pltpu.make_async_copy(ref, ref, sem).wait()


def grid_of(chips):
    tall = max(n for n in range(1, chips + 1) if chips % n == 0 and n * n <= chips)
    return tall, chips // tall


def kernel(
    seq, head,
    tok, wq, wk, wv, wo, out,
    x, normed, qkv, w, w_o, att, mixed, bias,
    tok_send, tok_recv, load_sem, z_send, z_recv, xy_send, xy_recv, far_recv, pair_recv,
    core_send, core_recv, out_send, out_recv,
):
    s, z = lax.axis_index("seq"), lax.axis_index("head")
    slots, frames = x.shape[0], x.shape[1]
    groups = tok.shape[1] // (seq * head * SUB)
    own_frames = tok.shape[0]
    width = tok.shape[2]
    columns = wq.shape[1]
    rows = frames * SUB
    slice_rows = width // seq
    half_rows = slice_rows // 2
    half_seq = seq // 2
    shard = width // head
    parity, place = lax.rem(s, 2), s // 2
    sibling = s + 1 - 2 * parity
    total = seq * head
    tall, wide = grid_of(half_seq)
    paired = tall == 2 and wide == 2
    up, across = place // wide, lax.rem(place, wide)
    colour = lax.rem(up + across, 2) if paired else 0
    colours = 2 if paired else 1
    sliced = (0, 1) if paired else (0, 1, 2)

    def send(src, dst, send_sem, recv_sem, to_s, to_z):
        pltpu.make_async_remote_copy(
            src_ref=src, dst_ref=dst, send_sem=send_sem, recv_sem=recv_sem,
            device_id=(to_s, to_z), device_id_type=MESH,
        ).start()

    def device_at(a, b):
        return (lax.rem(a, tall) * wide + lax.rem(b, wide)) * 2 + parity

    def slice_at(a, b, start, size):
        first = parity * half_seq + lax.rem(a, tall) * wide + lax.rem(b, wide)
        return pl.ds(pl.multiple_of(first * slice_rows + start, half_rows), size)

    def part(j):
        return (width if j < 3 else shard) // (2 * colours)

    def part_at(j, from_z, hue, start, size):
        first = (hue * 2 + parity) * part(j) + start
        if j < 3:
            return w.at[j, from_z, pl.ds(pl.multiple_of(first, size), size), :]
        return w_o.at[pl.ds(pl.multiple_of(from_z * shard + first, size), size), :]

    weights = (wq, wk, wv, wo)
    my_slice = slice_at(up, across, 0, slice_rows)

    def line_piece(j, from_z):
        if j in sliced:
            return w.at[j, from_z, my_slice, :]
        return part_at(j, from_z, colour, 0, part(j))

    def own_piece(j):
        if j in sliced:
            return weights[j].at[my_slice, :]
        start = pl.multiple_of((colour * 2 + parity) * part(j), part(j))
        return weights[j].at[pl.ds(start, part(j)), :]

    def ways(d):
        return (
            (z - d, z - d >= 0, z + 1, z + 1 < head),
            (z + d, z + d < head, z - 1, z - 1 >= 0),
        )

    def known(from_z):
        return jnp.clip(from_z, 0, head - 1)

    inner = (z > 0) & (z + 1 < head)
    deep = inner.astype(jnp.int32)
    uneven = head == 4 and paired and groups == 4
    edge_groups, full, twice = (3, 5, 0) if uneven else (groups, groups, 0)

    def whole(j, from_z, to_z):
        if not paired:
            return z < 0
        deep = (to_z > 0) & (to_z + 1 < head)
        if j == 3:
            return z < 0
        if j == 2:
            return deep
        return deep & ((from_z == 0) | (from_z == head - 1))

    def launch(j):
        for _, _, after, open_ in ways(1):

            @pl.when(open_)
            def _():
                send(own_piece(j), line_piece(j, z), z_send.at[j], z_recv.at[j, z], s, after)

    def complete(j):
        if not paired:
            return
        for _, _, after, open_ in ways(1):

            @pl.when(open_ & whole(j, z, after))
            def _():
                if j in sliced:
                    places = (
                        ((0, 1), xy_recv.at[j, 0, z]), ((1, 0), xy_recv.at[j, 1, z]),
                        ((1, 1), far_recv.at[j]),
                    )
                    for (a, b), arrived in places:
                        some = slice_at(up + a, across + b, 0, slice_rows)
                        send(
                            weights[j].at[some, :], w.at[j, z, some, :],
                            z_send.at[j], arrived, s, after,
                        )
                else:
                    size = part(j) // 2
                    for i in range(2):
                        first = ((1 - colour) * 2 + parity) * part(j) + i * size
                        send(
                            weights[j].at[pl.ds(pl.multiple_of(first, size), size), :],
                            part_at(j, z, 1 - colour, i * size, size),
                            z_send.at[j], pair_recv.at[j - 2, i, z], s, after,
                        )

    def picked(from_z, outer):
        edge = (from_z == 0) | (from_z == head - 1)
        if outer is None:
            return True
        return edge if outer else jnp.logical_not(edge)

    def arrive(j, d, outer=None):
        for from_z, valid, _, _ in ways(d):

            @pl.when(valid & picked(from_z, outer))
            def _():
                drain(line_piece(j, known(from_z)), z_recv.at[j, known(from_z)])

    def pass_on(j, d, outer=None):
        for from_z, valid, after, open_ in ways(d):

            @pl.when(valid & open_ & picked(from_z, outer))
            def _():
                piece = line_piece(j, known(from_z))
                send(piece, piece, z_send.at[j], z_recv.at[j, known(from_z)], s, after)

    def spread(j, d, outer=None):
        for from_z, valid, _, _ in ways(d):
            f = known(from_z)
            valid = valid & picked(from_z, outer)
            thin = valid & jnp.logical_not(whole(j, from_z, z)) if d == 1 else valid
            piece = line_piece(j, f)

            @pl.when(thin)
            def _():
                if j in sliced:
                    for k in range(1, wide):
                        to_s = device_at(up, across + k)
                        send(piece, piece, xy_send.at[j], xy_recv.at[j, k - 1, f], to_s, z)
                    for k in range(1, tall):
                        to_s = device_at(up + k, across)
                        send(piece, piece, xy_send.at[j], xy_recv.at[j, wide + k - 2, f], to_s, z)
                elif paired:
                    size = part(j) // 2
                    for i, to_s in ((0, device_at(up, across + 1)), (1, device_at(up + 1, across))):
                        some = part_at(j, f, colour, i * size, size)
                        send(some, some, xy_send.at[j], pair_recv.at[j - 2, i, f], to_s, z)

            if j not in sliced:

                @pl.when(valid)
                def _():
                    send(piece, piece, core_send.at[j], core_recv.at[j], sibling, z)

    def relay(j, d, full=False):
        for from_z, valid, _, _ in ways(d):
            f = known(from_z)
            if d == 1:
                is_whole = whole(j, from_z, z)
                chosen = valid & (is_whole if full else jnp.logical_not(is_whole))
            elif full:
                continue
            else:
                chosen = valid

            @pl.when(chosen)
            def _():
                if j in sliced:
                    for k in range(1, wide):
                        b = across + wide - k
                        drain(w.at[j, f, slice_at(up, b, 0, slice_rows), :], xy_recv.at[j, k - 1, f])
                        some = w.at[j, f, slice_at(up, b, 0, half_rows), :]
                        for n in range(1, 1 if full else tall):
                            to_s = device_at(up + n, across)
                            send(some, some, xy_send.at[j], far_recv.at[j], to_s, z)
                    for k in range(1, tall):
                        a = up + tall - k
                        drain(
                            w.at[j, f, slice_at(a, across, 0, slice_rows), :],
                            xy_recv.at[j, wide + k - 2, f],
                        )
                        some = w.at[j, f, slice_at(a, across, half_rows, half_rows), :]
                        for n in range(1, 1 if full else wide):
                            to_s = device_at(up, across + n)
                            send(some, some, xy_send.at[j], far_recv.at[j], to_s, z)
                    return
                if paired:
                    size = part(j) // 2
                    for i in range(2):
                        some = part_at(j, f, 1 - colour, i * size, size)
                        drain(some, pair_recv.at[j - 2, i, f])
                        send(some, some, core_send.at[j], core_recv.at[j], sibling, z)

    far = (tall - 1) * (wide - 1) * slice_rows
    parity_rows = pl.ds(
        pl.multiple_of(parity * half_seq * slice_rows, slice_rows), half_seq * slice_rows
    )

    def to_sibling(j):
        if j not in sliced:
            return
        if far:
            drain(w.at[j, pl.ds(0, head - 1), pl.ds(0, far), :], far_recv.at[j])
        for i in range(1, head):
            piece = w.at[j, lax.rem(z + i, head), parity_rows, :]
            send(piece, piece, core_send.at[j], core_recv.at[j], sibling, z)

    def patches_of(to_s, g):
        if not uneven:
            block = (z * seq + to_s) * groups + g
        else:
            at_edge = ((z // (head - 1)) * seq + to_s) * edge_groups + g
            single = 2 * seq * edge_groups + ((z - 1) * seq + to_s) * full + g
            double = 2 * seq * (edge_groups + full) + to_s * twice + (g - full)
            late = int(g >= full) if isinstance(g, int) else (g >= full).astype(jnp.int32)
            block = at_edge + deep * (single + late * (double - single) - at_edge)
        return pl.ds(pl.multiple_of(block * SUB, SUB), SUB)

    def tok_block(to_s, g):
        return tok.at[:, patches_of(to_s, g), :]

    def exchange(g):
        for i in range(1, seq):
            to_s = lax.rem(s + i, seq)
            send(
                tok_block(to_s, g), x.at[g, pl.ds(s * own_frames, own_frames)],
                tok_send.at[g], tok_recv.at[g], to_s, z,
            )

    def keep(g):
        pltpu.make_async_copy(
            tok_block(s, g), x.at[g, pl.ds(s * own_frames, own_frames)], tok_recv.at[g]
        ).start()

    barrier = pltpu.get_barrier_semaphore()
    for i in range(1, seq):
        pl.semaphore_signal(
            barrier, inc=1, device_id=(lax.rem(s + i, seq), z), device_id_type=MESH
        )
    for _, _, after, open_ in ways(1):

        @pl.when(open_)
        def _():
            pl.semaphore_signal(barrier, inc=1, device_id=(s, after), device_id_type=MESH)

    own = [pltpu.make_async_copy(weights[j], w.at[j, z], load_sem.at[j]) for j in range(3)]
    own.append(
        pltpu.make_async_copy(
            wo, w_o.at[pl.ds(pl.multiple_of(z * shard, shard), shard), :], load_sem.at[3]
        )
    )
    for copy in own:
        copy.start()
    keep(0)

    row = lax.broadcasted_iota(jnp.int32, (rows, rows), 0)
    col = lax.broadcasted_iota(jnp.int32, (rows, rows), 1)
    bias[...] = jnp.where((row & (SUB - 1)) == (col & (SUB - 1)), 0.0, MASKED)

    lines = (z > 0).astype(jnp.int32) + (z + 1 < head).astype(jnp.int32)
    pl.semaphore_wait(barrier, seq - 1 + lines)

    step_frames = 8

    def norm(g):
        drain(x.at[g], tok_recv.at[g])

        @pl.loop(0, frames // step_frames, unroll=True)
        def _(c):
            block = x[g, pl.ds(c * step_frames, step_frames)].astype(jnp.float32)
            values = block.reshape(step_frames * SUB, width)
            mean = jnp.mean(values, axis=-1, keepdims=True)
            centered = values - mean
            var = jnp.mean(centered * centered, axis=-1, keepdims=True)
            start = pl.multiple_of(c * step_frames * SUB, step_frames * SUB)
            normed[pl.ds(start, step_frames * SUB), :] = (
                centered * lax.rsqrt(var + EPSILON)
            ).astype(jnp.bfloat16)

    def project(j):
        @pl.loop(0, head, unroll=True)
        def _(h):
            r = jnp.dot(normed[...], w[j, h], preferred_element_type=jnp.float32)
            if j == 0:
                r = r * HS ** (-0.5)
            start = pl.multiple_of(h * columns, columns)
            qkv[j, :, pl.ds(start, columns)] = r.astype(jnp.bfloat16)

    def take(j):
        own[j].wait()
        if j < 3:
            drain(
                w.at[j, pl.ds(0, head - 1), pl.ds(0, width // 2), :], core_recv.at[j]
            )
            project(j)
        else:
            drain(w_o.at[pl.ds(0, (head - 1) * shard // 2), :], core_recv.at[j])

    pair = 2 * HS
    left = lax.broadcasted_iota(jnp.int32, (rows, pair), 1) < HS
    left_b = left.astype(jnp.float32).astype(jnp.bfloat16)
    right_b = (1.0 - left.astype(jnp.float32)).astype(jnp.bfloat16)
    ones = jnp.ones((rows, pair), jnp.bfloat16)

    def out_block(g):
        return out.at[:, patches_of(s, g), :]

    pairs = width // pair
    some = pairs // 2

    def attend(start, stop):
        @pl.loop(start, stop, unroll=4)
        def _(n):
            lanes = pl.ds(pl.multiple_of(n * pair, pair), pair)
            q, k, v = qkv[0, :, lanes], qkv[1, :, lanes], qkv[2, :, lanes]
            v_ones = jnp.concatenate([v, ones], axis=1)
            results = []
            for mask in (left_b, right_b):
                score = lax.dot_general(
                    q * mask, k, (((1,), (1,)), ((), ())), preferred_element_type=jnp.float32
                )
                score = score + bias[...]
                top = jnp.max(score, axis=1, keepdims=True)
                raised = jnp.exp(score - top).astype(jnp.bfloat16)
                r = jnp.dot(raised, v_ones, preferred_element_type=jnp.float32)
                results.append(r[:, :pair] / r[:, pair:])
            att[:, lanes] = jnp.where(left, results[0], results[1]).astype(jnp.bfloat16)

    if head == 4:
        order = (lax.rem(z + 2, 4), z + 1 - 2 * lax.rem(z, 2), 3 - z, z)
    else:
        order = tuple(lax.rem(z + k, head) for k in range(1, head)) + (z,)

    def blend(g, h):
        lanes = pl.ds(pl.multiple_of(h * columns, columns), columns)
        r = jnp.dot(att[...], w_o[:, lanes], preferred_element_type=jnp.float32)
        mixed[g, pl.ds(h * frames, frames)] = r.reshape(frames, SUB, columns).astype(jnp.bfloat16)

    def deliver(g, some_heads):
        for h in some_heads:

            @pl.loop(1 if h is z else 0, seq)
            def _(i):
                to_s = lax.rem(s + i, seq)
                send(
                    mixed.at[g, pl.ds(h * frames + to_s * own_frames, own_frames)],
                    out_block(g), out_send.at[g], out_recv, to_s, h,
                )

        pltpu.make_async_copy(
            mixed.at[g, pl.ds(z * frames + s * own_frames, own_frames)], out_block(g), out_recv
        ).start()

    def mix(g):
        for h in range(head):
            blend(g, h)
        deliver(g, order)

    def mix_half(g):
        for h in order[2:]:
            blend(g, h)
        deliver(g, order[2:])

    for j in range(3):
        launch(j)
    exchange(0)

    @pl.when(jnp.logical_not(inner))
    def _():
        launch(3)
        for j in range(3):
            complete(j)

    for j in (0, 1):
        arrive(j, 1)
        pass_on(j, 1)
        spread(j, 1)

    def fetch(g, count=edge_groups):
        if g < count:
            exchange(g)
            keep(g)

    def forward(j, d, outer=None):
        arrive(j, d, outer)
        pass_on(j, d, outer)
        spread(j, d, outer)

    @pl.when(inner)
    def _():
        launch(3)
        forward(2, 1, True)
        arrive(2, 1, False)
        spread(2, 1, False)
        norm(0)
        for d in range(2, head):
            for j in (0, 1):
                forward(j, d)
        pass_on(2, 1, False)
        forward(3, 1, True)
        for j in range(3):
            complete(j)
        for j in (0, 1):
            relay(j, 1)
        for j in (0, 1):
            for d in range(2, head):
                relay(j, d)
        for d in range(2, head):
            forward(2, d)
        forward(3, 1, False)
        relay(0, 1, True)
        to_sibling(0)
        for d in range(2, head):
            forward(3, d)
        relay(1, 1, True)
        to_sibling(1)
        fetch(1, full + twice)
        take(0)
        relay(2, 1)
        for d in range(2, head):
            relay(2, d)
        take(1)
        relay(2, 1, True)
        to_sibling(2)
        relay(3, 1)
        take(2)
        attend(0, some)
        for d in range(2, head):
            relay(3, d)
        relay(3, 1, True)
        fetch(2, full + twice)
        attend(some, pairs)
        take(3)
        mix(0)
        for g in range(3, slots):
            fetch(g, full + twice)

    @pl.when(jnp.logical_not(inner))
    def _():
        arrive(2, 1)
        spread(2, 1)
        norm(0)
        for d in range(2, head):
            for j in (0, 1):
                arrive(j, d)
                spread(j, d)
                relay(j, d - 1)
            if d == 2:
                arrive(3, 1)
                spread(3, 1)
        if head == 2:
            arrive(3, 1)
            spread(3, 1)
        relay(2, 1)
        for d in range(2, head):
            arrive(2, d)
            spread(2, d)
            if d == 2:
                for j in (0, 1):
                    relay(j, head - 1)
                relay(3, 1)
        if head == 2:
            relay(0, 1)
            relay(1, 1)
        to_sibling(0)
        to_sibling(1)
        for d in range(2, head):
            arrive(3, d)
            spread(3, d)
            relay(2, d)
            if d == 2:
                take(0)
        if head == 2:
            take(0)
        to_sibling(2)
        take(1)
        for d in range(2, head - 1):
            relay(3, d)
        fetch(1)
        take(2)
        attend(0, some)
        fetch(2)
        if head > 2:
            relay(3, head - 1)
        else:
            relay(3, 1)
        attend(some, pairs)
        fetch(3)
        take(3)
        mix(0)

    def prepare(g):
        norm(g)
        for j in range(3):
            project(j)
        attend(0, pairs)

    @pl.loop(1, edge_groups + deep * (full - edge_groups))
    def _(g):
        prepare(g)
        mix(g)

    if twice:

        @pl.loop(full, full + twice * deep)
        def _(g):
            prepare(g)
            mix_half(g)

    drain(out, out_recv)
    blocks = head * frames
    def sent(g, count):
        drain(mixed.at[g, pl.ds(0, count)], out_send.at[g])
        drain(x.at[g, pl.ds(0, frames - own_frames)], tok_send.at[g])

    every = blocks - blocks // total
    for g in range(min(edge_groups, full)):
        sent(g, every)
    if uneven:

        @pl.when(jnp.logical_not(inner))
        def _():
            for g in range(full, edge_groups):
                sent(g, every)

        @pl.when(inner)
        def _():
            for g in range(edge_groups, full):
                sent(g, every)
            for g in range(full, full + twice):
                sent(g, 2 * frames - own_frames)

    for j in range(4):
        matrix = w.at[j, 0] if j < 3 else w_o

        def returned(count, sem):
            if count:
                drain(matrix.at[pl.ds(0, count), :], sem)

        if j in sliced:
            line, others, over = slice_rows, (half_seq - 1) * slice_rows, (half_seq - 1) * slice_rows
        else:
            line, others, over = part(j), part(j), part(j) if paired else 0
        for d in range(head):
            for from_z, valid, after, open_ in ways(d):

                @pl.when(valid & open_)
                def _():
                    returned(line, z_send.at[j])

                if d == 0:

                    @pl.when(open_ & whole(j, z, after))
                    def _():
                        returned(others, z_send.at[j])
                else:
                    thin = valid & jnp.logical_not(whole(j, from_z, z)) if d == 1 else valid

                    @pl.when(thin)
                    def _():
                        returned(over, xy_send.at[j])

        for _ in range(1, head):
            returned((width if j < 3 else shard) // 2, core_send.at[j])


def local(tokens, w_query, w_key, w_value, w_out):
    seq, head = lax.axis_size("seq"), lax.axis_size("head")
    own_frames, patches, width = tokens.shape
    frames = own_frames * seq
    groups = patches // (seq * head * SUB)
    tall, wide = grid_of(seq // 2)
    rows = frames * SUB
    uneven = head == 4 and (tall, wide) == (2, 2) and groups == 4
    slots = 5 if uneven else groups
    columns = w_query.shape[1]
    bf16 = jnp.bfloat16
    dma = pltpu.SemaphoreType.DMA
    return pl.pallas_call(
        functools.partial(kernel, seq, head),
        out_shape=pltpu.VMEM((own_frames, patches, width // head), bf16),
        in_specs=[pl.BlockSpec(memory_space=pl.ANY)] * 5,
        out_specs=pl.BlockSpec(memory_space=pl.ANY),
        scratch_shapes=[
            pltpu.VMEM((slots, frames, SUB, width), bf16),
            pltpu.VMEM((rows, width), bf16),
            pltpu.VMEM((3, rows, width), bf16),
            pltpu.VMEM((3, head, width, columns), bf16),
            pltpu.VMEM((width, width), bf16),
            pltpu.VMEM((rows, width), bf16),
            pltpu.VMEM((slots, head * frames, SUB, width // head), bf16),
            pltpu.VMEM((rows, rows), jnp.float32),
            dma((slots,)), dma((slots,)), dma((4,)),
            dma((4,)), dma((4, head)), dma((4,)), dma((3, max(tall + wide - 2, 1), head)), dma((3,)),
            dma((2, 2, head)), dma((4,)), dma((4,)), dma((slots,)), dma,
        ],
        compiler_params=pltpu.CompilerParams(
            has_side_effects=True, collective_id=0, vmem_limit_bytes=58 * 1024 * 1024
        ),
    )(tokens, w_query, w_key, w_value, w_out)


def solution(mesh):
    return jax.shard_map(
        local,
        mesh=mesh,
        in_specs=(
            P("seq", None, None),
            P(None, "head"),
            P(None, "head"),
            P(None, "head"),
            P("head", None),
        ),
        out_specs=P("seq", None, "head"),
        check_vma=False,
    )
```
